512 devices in a mesh: coil: 32 (over x, z), frame: 16 (over y, core).
Axes of the slice: x: 4, y: 8, z: 8, core: 2. Of those that a mesh axis runs over, the one named last changes fastest.
Arguments:
- initial_image: float32 [256, 16, 2, 256], P('coil', 'frame'), may hold values from -3 to 3
- coil_maps: bfloat16 [32, 2, 256, 256], P('coil'), may hold values from -1.5 to 1.5
- samples: bfloat16 [32, 16, 18, 2, 256], P('coil', 'frame'), may hold values from -6 to 6
- blocks_used: int32 [16], P('frame'), may hold values from 1 to 18, 145 in all
- row_offset: int32 [16, 18], P('frame'), may hold values from 0 to 128
- col_offset: int32 [16, 18], P('frame'), may hold values from 0 to 128
- row_first: int32 [16, 18, 256], P('frame'), may hold values from 0 to 124
- col_first: int32 [16, 18, 256], P('frame'), may hold values from 0 to 124
- row_taps: bfloat16 [16, 18, 4, 256], P('frame'), may hold values from 0.099609375 to 0.59765625
- col_taps: bfloat16 [16, 18, 4, 256], P('frame'), may hold values from 0.099609375 to 0.59765625
Outputs:
- image: float32 [256, 16, 2, 256], P('coil', 'frame')
- misfit: float32 [2, 16], P(None, 'frame')
The draws below stay inside these ranges and needn't reach their ends.
Inputs may be any that keep to these rules, and one draw needn't show every extreme that they name: Blocks 0 to blocks_used minus one of the frame were acquired. `row_first`: the kernel's 4 rows lie inside the tile. `col_first`: the kernel's 4 columns lie inside the tile.
All inputs are finite; a program needn't handle non-finite values.
Results may differ from the reference program's by a relative error of at most 0.006.
Values may be sent and summed in bfloat16 or wider, within the bound.
No kernel may reach another device: no remote copies, remote signals or barrier semaphores. Data moves between devices by JAX's collectives and lax.ppermute only.
A program may use at most 64 MiB of HBM per device.

```python
import math
import jax
import jax.numpy as jnp
import numpy as np
from jax import lax

N = 256
COILS = 32
FRAMES = 16
NB = 18
BS = 256
TT = 128
KW = 4
ITERS = 2


def touch_ends(drawn, own_key, least, largest):
    longest = drawn.shape.index(max(drawn.shape))
    spots = []
    for shift in (0, 1):
        where = [jax.random.randint(jax.random.fold_in(own_key, axis), (), 0, length) for axis, length in enumerate(drawn.shape)]
        where[longest] = (where[longest] + shift) % drawn.shape[longest]
        spots.append(tuple(where))
    return drawn.at[spots[0]].set(least).at[spots[1]].set(largest)


def spiked(array, rng, source, target, parts, factor):
    def block_of(axis_at):
        return (jnp.arange(array.shape[axis_at]) // (array.shape[axis_at] // parts)).reshape((-1,) + (1,) * (array.ndim - 1 - axis_at))

    first = jax.random.permutation(rng, parts)[block_of(target)]
    far = (block_of(target) + parts // 2) % parts
    return jnp.where((block_of(source) == first) | (block_of(source) == far), factor * array, array)


def level_of(stream_key, shape, cuts, low, top_value):
    def one(position, blocks):
        draws = jax.random.uniform(jax.random.fold_in(jax.random.fold_in(stream_key, 6), position), (blocks,), jnp.float32, low / len(cuts), top_value / len(cuts))
        return jnp.repeat(jnp.exp(draws), shape[position] // blocks).reshape((-1,) + (1,) * (len(shape) - position - 1))

    factor_of = one(*cuts[0])
    for cut in cuts[1:]:
        factor_of = factor_of * one(*cut)
    return factor_of


def length_profile(count, total, most, slope):
    portions = [(1 << 20) // math.isqrt(standing ** slope) + 1 for standing in range(2, count + 1)]
    rest, counts = total - most - (count - 1), [1] * (count - 1)
    while rest > 0:
        candidates = [i for i in range(count - 1) if counts[i] < most]
        mass, remaining = sum([portions[i] for i in candidates]), rest
        for i in candidates:
            addition = min(most - counts[i], max(1, remaining * portions[i] // mass), rest)
            counts[i] = counts[i] + addition
            rest = rest - addition
    return np.array([most] + counts)


def uneven_parts(stream_key, count, total, reach, lean):
    if count == 2:
        one = jax.random.randint(stream_key, (), max(1, total - reach), min(reach, total - 1) + 1)
        return jnp.stack([one, total - one])
    lengths = jnp.asarray(length_profile(count, total, reach, lean), jnp.int32)
    twos = (count - 1) // 2
    giver, sink = lengths[1:1 + 2 * twos:2], lengths[2:2 + 2 * twos:2]
    slack = jnp.minimum(giver - 1, reach - sink)
    passed = jax.random.randint(jax.random.fold_in(stream_key, 1), (twos,), 0, 1 << 20) % (slack + 1)
    lengths = lengths.at[1:1 + 2 * twos:2].set(giver - passed).at[2:2 + 2 * twos:2].set(sink + passed)
    return lengths[jax.random.permutation(jax.random.fold_in(stream_key, 2), count)]


def centred(rng, shape, width, most, shards=(), kind=jnp.bfloat16):
    gain = level_of(rng, shape, shards, -0.22, 0.18) if shards else 1.0
    drawn = jax.random.normal(rng, shape, jnp.float32) * width * gain
    return jnp.minimum(jnp.maximum(drawn, -most), most).astype(kind)


def bell_draw_with(stream_key, shape, deviation, most, shards, heavy, kind=jnp.bfloat16):
    entries = deviation * jax.random.normal(stream_key, shape, jnp.float32)
    if shards:
        entries = entries * level_of(stream_key, shape, shards, -0.22, 0.18)
    return jnp.clip(spiked(entries, jax.random.fold_in(stream_key, 3), *heavy), -most, most).astype(kind)


def setup_inputs(seed: int = 0) -> dict:
    key_list = jax.random.split(jax.random.key(seed), 11)
    return {
        "initial_image": centred(key_list[0], (N, FRAMES, 2, N), 0.5, 3.0, ((0, 32), (1, 16)), jnp.float32),
        "coil_maps": bell_draw_with(key_list[1], (COILS, 2, N, N), (2 * COILS) ** -0.5, 1.5, ((0, 32),), (0, 2, 32, 2.75)),
        "samples": centred(key_list[2], (COILS, FRAMES, NB, 2, BS), 1.0, 6.0, ((0, 32), (1, 16))),
        "blocks_used": uneven_parts(key_list[3], FRAMES, FRAMES * NB // 2 + 1, NB, 2).astype(jnp.int32),
        "row_offset": touch_ends(jax.random.randint(key_list[4], (FRAMES, NB), 0, N - TT + 1), jax.random.fold_in(key_list[4], 1), 0, N - TT).astype(jnp.int32),
        "col_offset": touch_ends(jax.random.randint(key_list[5], (FRAMES, NB), 0, N - TT + 1), jax.random.fold_in(key_list[5], 1), 0, N - TT).astype(jnp.int32),
        "row_first": touch_ends(jax.random.randint(key_list[6], (FRAMES, NB, BS), 0, TT - KW + 1), jax.random.fold_in(key_list[6], 1), 0, TT - KW).astype(jnp.int32),
        "col_first": touch_ends(jax.random.randint(key_list[7], (FRAMES, NB, BS), 0, TT - KW + 1), jax.random.fold_in(key_list[7], 1), 0, TT - KW).astype(jnp.int32),
        "row_taps": jnp.clip(0.099609375 + 0.49804688 * jax.random.uniform(key_list[8], (FRAMES, NB, KW, BS), jnp.float32) ** level_of(key_list[8], (FRAMES, NB, KW, BS), ((0, 16),), -0.2, 0.2), 0.099609375, 0.59765625).astype(jnp.bfloat16),
        "col_taps": jnp.clip(0.099609375 + 0.49804688 * jax.random.uniform(key_list[9], (FRAMES, NB, KW, BS), jnp.float32) ** level_of(key_list[9], (FRAMES, NB, KW, BS), ((0, 16),), -0.2, 0.2), 0.099609375, 0.59765625).astype(jnp.bfloat16),
    }


step_size = 2.0
tv_weight = 0.1
smooth_floor = 0.5
shrink_weight = 0.1

def rounded(values):
    return lax.optimization_barrier(values.astype(jnp.bfloat16))

def pair_tables(order):
    counter = jnp.arange(order, dtype=jnp.int32)
    phase = counter[:, None] * counter[None, :] % order
    angle = phase.astype(jnp.float32) * (2.0 * math.pi / order)
    cosine = (jnp.cos(angle) / math.sqrt(order)).astype(jnp.bfloat16)
    sine = (jnp.sin(angle) / math.sqrt(order)).astype(jnp.bfloat16)
    table_one = jnp.stack([jnp.stack([cosine, sine]), jnp.stack([-sine, cosine])])
    table_two = jnp.stack([jnp.stack([cosine, -sine]), jnp.stack([sine, cosine])])
    return (table_one, table_two)

def tap_matrix(first_idx, taps):
    positions = jnp.arange(TT, dtype=jnp.int32)
    matrix = jnp.zeros((first_idx.shape[0], TT), jnp.float32)
    for offset in range(KW):
        hits = positions[None, :] == first_idx[:, None] + offset
        matrix = matrix + jnp.where(hits, taps[offset].astype(jnp.float32)[:, None], 0.0)
    return matrix.astype(jnp.bfloat16)

def spoke_block(kspace, grid_sum, tile_row, tile_col, first_row, first_col, taps_row, taps_col, measured, active):
    rows_matrix = tap_matrix(first_row, taps_row)
    cols_matrix = tap_matrix(first_col, taps_col)
    anchor = jnp.zeros((), jnp.int32)
    corner = (anchor, tile_row.astype(jnp.int32), tile_col.astype(jnp.int32))
    grid_tile = lax.dynamic_slice(kspace, corner, (2, TT, TT))
    across = jnp.einsum('si,pij->psj', rows_matrix.astype(jnp.float32), grid_tile.astype(jnp.float32))
    cols_wide = cols_matrix.astype(jnp.float32)
    predicted = lax.optimization_barrier(jnp.sum(across * cols_wide[None], axis=2))
    resid = (predicted - measured.astype(jnp.float32)) * active
    misfit = jnp.sum(resid * resid)
    resid_low = rounded(resid)
    weighted = rounded(resid_low.astype(jnp.float32)[:, :, None] * cols_wide[None])
    spread = jnp.einsum('si,psj->pij', rows_matrix.astype(jnp.float32), weighted.astype(jnp.float32))
    updated = lax.dynamic_slice(grid_sum, corner, (2, TT, TT)) + spread
    return (lax.dynamic_update_slice(grid_sum, updated, corner), misfit)

def frame_grid(kspace, count, row_off, col_off, row_idx, col_idx, row_w, col_w, measured):

    def visit(running, inputs):
        grid_sum, misfit_sum = running
        block_id, tile_row, tile_col, first_row, first_col, taps_row, taps_col, block_data = inputs
        active = (block_id < count).astype(jnp.float32)
        grid_sum, misfit = spoke_block(kspace, grid_sum, tile_row, tile_col, first_row, first_col, taps_row, taps_col, block_data, active)
        return ((grid_sum, misfit_sum + misfit), None)
    initial = (jnp.zeros((2, N, N), jnp.float32), jnp.zeros((), jnp.float32))
    blocks = jnp.arange(NB, dtype=jnp.int32)
    (grid_sum, misfit_sum), unused = lax.scan(visit, initial, (blocks, row_off, col_off, row_idx, col_idx, row_w, col_w, measured))
    return (rounded(grid_sum), misfit_sum)

def coil_forward(image_low, maps, table_one, table_two):
    maps_wide = maps.astype(jnp.float32)
    image_wide = image_low.astype(jnp.float32)
    real_part = maps_wide[0][:, None, :] * image_wide[:, :, 0] - maps_wide[1][:, None, :] * image_wide[:, :, 1]
    imag_part = maps_wide[0][:, None, :] * image_wide[:, :, 1] + maps_wide[1][:, None, :] * image_wide[:, :, 0]
    coil_image = rounded(jnp.stack([real_part, imag_part], axis=2))
    half = rounded(jnp.einsum('qprk,kfpn->fqrn', table_one.astype(jnp.float32), coil_image.astype(jnp.float32)))
    return rounded(jnp.einsum('fprk,pqkn->fqrn', half.astype(jnp.float32), table_two.astype(jnp.float32)))

def coil_adjoint(grid_low, maps, table_one, table_two):
    back_half = rounded(jnp.einsum('qprk,fpkn->fqrn', table_two.astype(jnp.float32), grid_low.astype(jnp.float32)))
    coil_back = jnp.einsum('fprk,pqkn->rfqn', back_half.astype(jnp.float32), table_one.astype(jnp.float32))
    maps_wide = maps.astype(jnp.float32)
    real_part = maps_wide[0][:, None, :] * coil_back[:, :, 0] + maps_wide[1][:, None, :] * coil_back[:, :, 1]
    imag_part = maps_wide[0][:, None, :] * coil_back[:, :, 1] - maps_wide[1][:, None, :] * coil_back[:, :, 0]
    return jnp.stack([real_part, imag_part], axis=2)

def cine_gradient(padded):
    change = padded[:, 1:] - padded[:, :-1]
    length = jnp.sqrt(lax.optimization_barrier(jnp.sum(change * change, axis=2, keepdims=True)) + smooth_floor * smooth_floor)
    normed = change / length
    return normed[:, :-1] - normed[:, 1:]

def shrink(detail, limit):
    length = jnp.sqrt(lax.optimization_barrier(jnp.sum(detail * detail, axis=2, keepdims=True)))
    return detail * (jnp.maximum(length - limit, 0.0) / jnp.maximum(length, limit))

def wavelet_prox(field, limit):
    even_rows = field[0::2]
    odd_rows = field[1::2]
    top_left = even_rows[..., 0::2]
    top_right = even_rows[..., 1::2]
    low_left = odd_rows[..., 0::2]
    low_right = odd_rows[..., 1::2]
    approx = (top_left + top_right + low_left + low_right) * 0.5
    horiz = shrink((top_left - top_right + low_left - low_right) * 0.5, limit)
    vertical = shrink((top_left + top_right - low_left - low_right) * 0.5, limit)
    diagonal = shrink((top_left - top_right - low_left + low_right) * 0.5, limit)
    new_tl = (approx + horiz + vertical + diagonal) * 0.5
    new_tr = (approx - horiz + vertical - diagonal) * 0.5
    new_ll = (approx + horiz - vertical - diagonal) * 0.5
    new_lr = (approx - horiz - vertical + diagonal) * 0.5
    top_rows = jnp.stack([new_tl, new_tr], axis=-1).reshape(even_rows.shape)
    low_rows = jnp.stack([new_ll, new_lr], axis=-1).reshape(odd_rows.shape)
    return jnp.stack([top_rows, low_rows], axis=1).reshape(field.shape)

def reference(initial_image, coil_maps, samples, blocks_used, row_offset, col_offset, row_first, col_first, row_taps, col_taps):
    table_one, table_two = pair_tables(N)
    grid_frames = jax.vmap(frame_grid)

    def data_term(image_low):

        def per_coil(running, inputs):
            grad_sum, misfit_sum = running
            maps, measured = inputs
            kspace = coil_forward(image_low, maps, table_one, table_two)
            grid_low, misfit = grid_frames(kspace, blocks_used, row_offset, col_offset, row_first, col_first, row_taps, col_taps, measured)
            partial_image = coil_adjoint(grid_low, maps, table_one, table_two)
            return ((grad_sum + partial_image, misfit_sum + misfit), None)
        initial = (jnp.zeros(initial_image.shape, jnp.float32), jnp.zeros((FRAMES,), jnp.float32))
        totals, unused = lax.scan(per_coil, initial, (coil_maps, samples))
        return totals
    misfit_scale = 0.5 / (COILS * NB * BS)
    current = initial_image.astype(jnp.float32)
    moving = current
    momentum = 1.0
    misfit_rows = []
    for step_num in range(ITERS):
        data_grad, misfit = data_term(rounded(moving))
        misfit_rows.append(misfit * misfit_scale)
        padded = jnp.concatenate([moving[:, -1:], moving, moving[:, :1]], axis=1)
        descent = moving - step_size * (data_grad + tv_weight * cine_gradient(padded))
        updated = wavelet_prox(descent, step_size * shrink_weight)
        following = (1.0 + math.sqrt(1.0 + 4.0 * momentum * momentum)) / 2.0
        moving = updated + (momentum - 1.0) / following * (updated - current)
        current = updated
        momentum = following
    return (current, jnp.stack(misfit_rows))
```

```python
import math

import jax
import jax.numpy as jnp
import numpy as np
from jax import lax
from jax.experimental import pallas as pl
from jax.experimental.pallas import tpu as pltpu
from jax.sharding import PartitionSpec as P

N = 256
NB = 18
BS = 256
KW = 4
ITERS = 2
GROUP = 2
NG = NB // GROUP
GS = GROUP * BS

step_size = 2.0
tv_weight = 0.1
smooth_floor = 0.5
shrink_weight = 0.1

f32 = jnp.float32
bf16 = jnp.bfloat16


def pair_tables(order):
    counter = np.arange(order)
    phase = (counter[:, None] * counter[None, :]) % order
    angle = phase.astype(np.float32) * np.float32(2.0 * math.pi / order)
    cosine = np.cos(angle) / np.float32(math.sqrt(order))
    sine = np.sin(angle) / np.float32(math.sqrt(order))
    forward = np.block([[cosine, sine], [-sine, cosine]])
    return jnp.asarray(forward, bf16), jnp.asarray(forward.T, bf16)


def vmem():
    return pl.BlockSpec(memory_space=pltpu.VMEM)


def smem():
    return pl.BlockSpec(memory_space=pltpu.SMEM)


def anywhere():
    return pl.BlockSpec(memory_space=pl.ANY)


def dot(left, right):
    return lax.dot_general(left, right, (((1,), (0,)), ((), ())), preferred_element_type=f32)


def dot_nt(left, right):
    return lax.dot_general(left, right, (((1,), (1,)), ((), ())), preferred_element_type=f32)


def start_kernel(image_ref, send_ref, rows_ref):
    real = image_ref[:, 0, 0, :]
    imag = image_ref[:, 0, 1, :]
    rows_ref[:, :N] = real
    rows_ref[:, N:] = imag
    low = jnp.concatenate([real, imag], axis=1).astype(bf16)
    send_ref[...] = jnp.broadcast_to(low[None], send_ref.shape)


def taps_kernel(count_ref, row_off_ref, col_off_ref, row_first_ref, col_first_ref, row_taps_ref, col_taps_ref, wx_ref, wy_ref):
    groups = (count_ref[0] + GROUP - 1) // GROUP
    position = lax.broadcasted_iota(jnp.int32, (N, BS), 0)

    def build(start, taps):
        matrix = jnp.zeros((N, BS), f32)
        for tap in range(KW):
            matrix = jnp.where(position == start + tap, taps[tap : tap + 1], matrix)
        return matrix.astype(bf16)

    def visit(group, carry):
        for member in range(GROUP):
            block = group * GROUP + member
            lanes = slice(member * BS, (member + 1) * BS)
            row_start = row_first_ref[0, pl.ds(block, 1), :] + row_off_ref[0, block]
            col_start = col_first_ref[0, pl.ds(block, 1), :] + col_off_ref[0, block]
            wx_ref[group, :, lanes] = build(row_start, row_taps_ref[0, block].astype(f32))
            wy_ref[group, :, lanes] = build(col_start, col_taps_ref[0, block].astype(f32))
        return carry

    lax.fori_loop(0, groups, visit, 0)


def pieces(value):
    high = value.astype(bf16)
    rest = value - high.astype(f32)
    middle = rest.astype(bf16)
    low = (rest - middle.astype(f32)).astype(bf16)
    return high.astype(f32), middle.astype(f32), low.astype(f32)


def coil_kernel(last, *refs):
    if last:
        (count_ref, image_ref, maps_ref, samples_ref, fwd_ref, adj_ref, wx_hbm, wy_hbm, before_ref) = refs[:9]
        (send_ref, wx_ref, wy_ref, grid_ref, sems) = refs[9:]
    else:
        (count_ref, image_ref, maps_ref, samples_ref, fwd_ref, adj_ref, wx_hbm, wy_hbm) = refs[:8]
        (send_ref, misfit_ref, wx_ref, wy_ref, grid_ref, sems) = refs[8:]
    count = count_ref[0]
    groups = (count + GROUP - 1) // GROUP

    def copies(group):
        return (
            pltpu.make_async_copy(wx_hbm.at[group], wx_ref.at[group], sems.at[0, group]),
            pltpu.make_async_copy(wy_hbm.at[group], wy_ref.at[group], sems.at[1, group]),
        )

    def fetch(group, carry):
        for copy in copies(group):
            copy.start()
        return carry

    lax.fori_loop(0, groups, fetch, 0)

    image = image_ref[...].astype(f32)
    real = image[:, :, :N].reshape(N, N)
    imag = image[:, :, N:].reshape(N, N)
    map_real = maps_ref[0, 0].astype(f32)
    map_imag = maps_ref[0, 1].astype(f32)
    coil_real = (map_real * real - map_imag * imag).astype(bf16)
    coil_imag = (map_real * imag + map_imag * real).astype(bf16)
    coil_image = jnp.concatenate([coil_real, coil_imag], axis=0)
    half = dot(fwd_ref[...], coil_image).astype(bf16)
    half = jnp.concatenate([half[:N], half[N:]], axis=1)
    kspace = dot_nt(fwd_ref[...], half).astype(bf16)
    grid_ref[...] = jnp.zeros_like(grid_ref)

    def visit(group, misfit):
        for copy in copies(group):
            copy.wait()
        wx = wx_ref[group]
        wy = wy_ref[group]
        wy_wide = wy.astype(f32)
        across = dot(kspace, wx)
        weighted = []
        for part in range(2):
            predicted = jnp.sum(across[part * N : (part + 1) * N] * wy_wide, axis=0, keepdims=True)
            resid = []
            for member in range(GROUP):
                block = group * GROUP + member
                measured = samples_ref[0, 0, block].astype(f32)[part : part + 1]
                off = predicted[:, member * BS : (member + 1) * BS] - measured
                resid.append(jnp.where(block < count, off, 0.0))
            resid = jnp.concatenate(resid, axis=1)
            misfit = misfit + resid * resid
            weighted.append(wy * resid.astype(bf16))
        weighted = jnp.concatenate(weighted, axis=0)
        grid_ref[...] += dot_nt(weighted, wx)
        return misfit

    misfit = lax.fori_loop(0, groups, visit, jnp.zeros((1, GS), f32))
    misfit = jnp.broadcast_to(jnp.sum(misfit, axis=1, keepdims=True), (8, 128))

    grid = grid_ref[...].astype(bf16)
    grid = jnp.concatenate([grid[:N], grid[N:]], axis=1)
    back_half = dot_nt(adj_ref[...], grid).astype(bf16)
    back_half = jnp.concatenate([back_half[:N], back_half[N:]], axis=1)
    back = dot(back_half, fwd_ref[...])
    back_real = back[:, :N]
    back_imag = back[:, N:]
    out_real = map_real * back_real + map_imag * back_imag
    out_imag = map_real * back_imag - map_imag * back_real
    parts = send_ref.shape[0]
    send_ref[:, :, :N] = out_real.reshape(parts, -1, N).astype(bf16)
    send_ref[:, :, N : 2 * N] = out_imag.reshape(parts, -1, N).astype(bf16)
    if last:
        row = lax.broadcasted_iota(jnp.int32, (8, 128), 0)
        extra = jnp.zeros((8, 128), f32)
        for place, piece in enumerate(pieces(before_ref[...]) + pieces(misfit)):
            extra = jnp.where(row == place, piece, extra)
        send_ref[:, :, 2 * N :] = jnp.broadcast_to(extra.astype(bf16)[None], (parts, 8, 128))
    else:
        misfit_ref[...] = misfit


def shrunk(detail, limit):
    real = detail[:, :N]
    imag = detail[:, N:]
    length = jnp.sqrt(real * real + imag * imag)
    factor = jnp.maximum(length - limit, 0.0) / jnp.maximum(length, limit)
    return detail * jnp.concatenate([factor, factor], axis=1)


def unit_change(change):
    real = change[:, :N]
    imag = change[:, N:]
    length = jnp.sqrt(real * real + imag * imag + smooth_floor * smooth_floor)
    return change / jnp.concatenate([length, length], axis=1)


def update_kernel(last, carry_on, misfit_scale, *refs):
    if last:
        (parts_ref, moving_ref, left_ref, right_ref, image_ref, misfit_ref) = refs
    else:
        (parts_ref, moving_ref, left_ref, right_ref, current_ref, send_ref, updated_ref, next_ref) = refs
    total = jnp.sum(parts_ref[...].astype(f32), axis=0)
    moving = moving_ref[...]
    tv_grad = unit_change(moving - left_ref[...]) - unit_change(right_ref[...] - moving)
    field = moving - step_size * (total[:, : 2 * N] + tv_weight * tv_grad)
    rows, width = field.shape
    row_even = lax.broadcasted_iota(jnp.int32, field.shape, 0) % 2 == 0
    col_even = lax.broadcasted_iota(jnp.int32, field.shape, 1) % 2 == 0
    beside = jnp.where(col_even, pltpu.roll(field, width - 1, 1), pltpu.roll(field, 1, 1))
    col_sum = field + beside
    col_diff = jnp.where(col_even, field - beside, beside - field)

    def other_row(values):
        return jnp.where(row_even, pltpu.roll(values, rows - 1, 0), pltpu.roll(values, 1, 0))

    sum_other = other_row(col_sum)
    diff_other = other_row(col_diff)
    limit = step_size * shrink_weight
    approx = (col_sum + sum_other) * 0.5
    horiz = shrunk((col_diff + diff_other) * 0.5, limit)
    vertical = shrunk(jnp.where(row_even, col_sum - sum_other, sum_other - col_sum) * 0.5, limit)
    diagonal = shrunk(jnp.where(row_even, col_diff - diff_other, diff_other - col_diff) * 0.5, limit)
    across = jnp.where(row_even, horiz + diagonal, horiz - diagonal)
    along = jnp.where(row_even, approx + vertical, approx - vertical)
    updated = jnp.where(col_even, along + across, along - across) * 0.5
    if last:
        image_ref[:, 0, 0, :] = updated[:, :N]
        image_ref[:, 0, 1, :] = updated[:, N:]
        extra = total[:, 2 * N :] * misfit_scale
        misfit_ref[0:1, :] = jnp.sum(extra[0:3], axis=0, keepdims=True)
        misfit_ref[1:2, :] = jnp.sum(extra[3:6], axis=0, keepdims=True)
    else:
        following = updated + carry_on * (updated - current_ref[...])
        updated_ref[...] = updated
        next_ref[...] = following
        send_ref[...] = jnp.broadcast_to(following.astype(bf16)[None], send_ref.shape)


def exchanged(parts):
    return lax.all_to_all(parts, "coil", 0, 0, tiled=True)


def neighbours(values):
    count = lax.axis_size("frame")
    left = lax.ppermute(values, "frame", [(i, (i + 1) % count) for i in range(count)])
    right = lax.ppermute(values, "frame", [((i + 1) % count, i) for i in range(count)])
    return left, right


def on_device(
    initial_image,
    coil_maps,
    samples,
    blocks_used,
    row_offset,
    col_offset,
    row_first,
    col_first,
    row_taps,
    col_taps,
):
    coils = lax.axis_size("coil")
    rows = initial_image.shape[0]
    misfit_scale = 0.5 / (coil_maps.shape[0] * coils * NB * BS)
    forward, adjoint = pair_tables(N)
    params = pltpu.CompilerParams(vmem_limit_bytes=32 * 1024 * 1024)
    shape = jax.ShapeDtypeStruct
    send_shape = shape((coils, rows, 2 * N), bf16)
    rows_shape = shape((rows, 2 * N), f32)

    send, moving = pl.pallas_call(
        start_kernel,
        out_shape=(send_shape, rows_shape),
        in_specs=[vmem()],
        out_specs=(vmem(), vmem()),
        compiler_params=params,
        name="start",
    )(initial_image)
    current = moving

    wx, wy = pl.pallas_call(
        taps_kernel,
        out_shape=(shape((NG, N, GS), bf16), shape((NG, N, GS), bf16)),
        in_specs=[smem(), smem(), smem(), vmem(), vmem(), vmem(), vmem()],
        out_specs=(vmem(), vmem()),
        compiler_params=params,
        name="taps",
    )(blocks_used, row_offset, col_offset, row_first, col_first, row_taps, col_taps)

    momentum = 1.0
    misfit = None
    for step_num in range(ITERS):
        last = step_num == ITERS - 1
        gathered = exchanged(send)
        left, right = neighbours(moving)
        if step_num == 0:
            gathered, left, right, wx, wy = lax.optimization_barrier((gathered, left, right, wx, wy))
        else:
            gathered, left, right = lax.optimization_barrier((gathered, left, right))
        inputs = [blocks_used, gathered, coil_maps, samples, forward, adjoint, wx, wy]
        specs = [smem(), vmem(), vmem(), vmem(), vmem(), vmem(), anywhere(), anywhere()]
        if last:
            inputs.append(misfit)
            specs.append(vmem())
            out_shape = (shape((coils, rows, 2 * N + 128), bf16),)
        else:
            out_shape = (send_shape, shape((8, 128), f32))
        results = pl.pallas_call(
            lambda *refs, last=last: coil_kernel(last, *refs),
            out_shape=out_shape,
            in_specs=specs,
            out_specs=tuple(vmem() for _ in out_shape),
            scratch_shapes=[
                pltpu.VMEM((NG, N, GS), bf16),
                pltpu.VMEM((NG, N, GS), bf16),
                pltpu.VMEM((2 * N, N), f32),
                pltpu.SemaphoreType.DMA((2, NG)),
            ],
            compiler_params=params,
            name=f"coil{step_num}",
        )(*inputs)
        partial = results[0]
        if not last:
            misfit = results[1]
        parts = exchanged(partial)
        following = (1.0 + math.sqrt(1.0 + 4.0 * momentum * momentum)) / 2.0
        carry_on = (momentum - 1.0) / following
        inputs = [parts, moving, left, right]
        if last:
            out_shape = (shape(initial_image.shape, f32), shape((ITERS, 128), f32))
        else:
            inputs.append(current)
            out_shape = (send_shape, rows_shape, rows_shape)
        results = pl.pallas_call(
            lambda *refs, last=last, carry_on=carry_on: update_kernel(last, carry_on, misfit_scale, *refs),
            out_shape=out_shape,
            in_specs=[vmem() for _ in inputs],
            out_specs=tuple(vmem() for _ in out_shape),
            compiler_params=params,
            name=f"update{step_num}",
        )(*inputs)
        if last:
            image, misfit_rows = results
        else:
            send, current, moving = results
        momentum = following
    return image, misfit_rows[:, :1]


def solution(mesh):
    placed = (
        P("coil", "frame", None, None),
        P("coil", None, None, None),
        P("coil", "frame", None, None, None),
        P("frame"),
        P("frame", None),
        P("frame", None),
        P("frame", None, None),
        P("frame", None, None),
        P("frame", None, None, None),
        P("frame", None, None, None),
    )
    return jax.shard_map(
        on_device,
        mesh=mesh,
        in_specs=placed,
        out_specs=(P("coil", "frame", None, None), P(None, "frame")),
        check_vma=False,
    )
```

```python
import math

import jax
import jax.numpy as jnp
import numpy as np
from jax import lax
from jax.experimental import pallas as pl
from jax.experimental.pallas import tpu as pltpu
from jax.sharding import PartitionSpec as P

N = 256
NB = 18
BS = 256
KW = 4
ITERS = 2
GROUP = 2
NG = NB // GROUP
GS = GROUP * BS

step_size = 2.0
tv_weight = 0.1
smooth_floor = 0.5
shrink_weight = 0.1

f32 = jnp.float32
bf16 = jnp.bfloat16


def pair_table(order):
    counter = np.arange(order)
    phase = (counter[:, None] * counter[None, :]) % order
    angle = phase.astype(np.float32) * np.float32(2.0 * math.pi / order)
    cosine = np.cos(angle) / np.float32(math.sqrt(order))
    sine = np.sin(angle) / np.float32(math.sqrt(order))
    return jnp.asarray(np.block([[cosine, sine], [-sine, cosine]]), bf16)


def vmem():
    return pl.BlockSpec(memory_space=pltpu.VMEM)


def smem():
    return pl.BlockSpec(memory_space=pltpu.SMEM)


def hbm():
    return pl.BlockSpec(memory_space=pltpu.HBM)


def in_hbm(values):
    return pltpu.with_memory_space_constraint(values, pltpu.HBM)


def dot(left, right):
    return lax.dot_general(left, right, (((1,), (0,)), ((), ())), preferred_element_type=f32)


def dot_nt(left, right):
    return lax.dot_general(left, right, (((1,), (1,)), ((), ())), preferred_element_type=f32)


def start_kernel(image_hbm, send_ref, rows_ref, image_ref, sem):
    copy = pltpu.make_async_copy(image_hbm, image_ref, sem)
    copy.start()
    copy.wait()
    real = image_ref[:, 0, 0, :]
    imag = image_ref[:, 0, 1, :]
    rows_ref[:, :N] = real
    rows_ref[:, N:] = imag
    low = jnp.concatenate([real, imag], axis=1).astype(bf16)
    send_ref[...] = jnp.broadcast_to(low[None], send_ref.shape)


def taps_kernel(count_ref, *refs):
    sources, (wx_hbm, wy_hbm), kept, held = refs[:9], refs[9:11], refs[11:14], refs[14:20]
    wx_ref, wy_ref, in_sems, out_sems = refs[20:]
    row_off, col_off, row_first, col_first, row_taps, col_taps = held
    loads = [pltpu.make_async_copy(source, own, in_sems.at[k]) for k, (source, own) in enumerate(zip(sources, held + kept))]
    for load in loads:
        load.start()
    for load in loads[: len(held)]:
        load.wait()
    groups = (count_ref[0] + GROUP - 1) // GROUP
    position = lax.broadcasted_iota(jnp.int32, (N, BS), 0)

    def stores(group):
        return (
            pltpu.make_async_copy(wx_ref.at[group], wx_hbm.at[group], out_sems.at[0, group]),
            pltpu.make_async_copy(wy_ref.at[group], wy_hbm.at[group], out_sems.at[1, group]),
        )

    def build(start, taps):
        offset = position - start
        matrix = jnp.zeros((N, BS), f32)
        for tap in range(KW):
            matrix = jnp.where(offset == tap, taps[tap : tap + 1], matrix)
        return matrix.astype(bf16)

    def visit(group, carry):
        for member in range(GROUP):
            block = group * GROUP + member
            lanes = slice(member * BS, (member + 1) * BS)
            row_start = row_first[block] + row_off[0, block]
            col_start = col_first[block] + col_off[0, block]
            wx_ref[group, :, lanes] = build(row_start, row_taps[0, block].astype(f32))
            wy_ref[group, :, lanes] = build(col_start, col_taps[0, block].astype(f32))
        for store in stores(group):
            store.start()
        return carry

    lax.fori_loop(0, groups, visit, 0)

    def finish(group, carry):
        for store in stores(group):
            store.wait()
        return carry

    lax.fori_loop(0, groups, finish, 0)
    for load in loads[len(held) :]:
        load.wait()


def pieces(value):
    high = value.astype(bf16)
    rest = value - high.astype(f32)
    middle = rest.astype(bf16)
    low = (rest - middle.astype(f32)).astype(bf16)
    return high.astype(f32), middle.astype(f32), low.astype(f32)


def coil_kernel(last, *refs):
    if last:
        (count_ref, image_ref, maps_ref, samples_ref, fwd_ref, wx_hbm, wy_hbm, before_ref) = refs[:8]
        (send_ref, wx_ref, wy_ref, grid_ref, sems) = refs[8:]
    else:
        (count_ref, image_ref, maps_ref, samples_ref, fwd_ref, wx_hbm, wy_hbm) = refs[:7]
        (send_ref, misfit_ref, wx_ref, wy_ref, grid_ref, sems) = refs[7:]
    count = count_ref[0]
    groups = (count + GROUP - 1) // GROUP

    def copies(group):
        return (
            pltpu.make_async_copy(wx_hbm.at[group], wx_ref.at[group], sems.at[0, group]),
            pltpu.make_async_copy(wy_hbm.at[group], wy_ref.at[group], sems.at[1, group]),
        )

    def fetch(group, carry):
        for copy in copies(group):
            copy.start()
        return carry

    lax.fori_loop(0, groups, fetch, 0)

    image = image_ref[...].astype(f32)
    real = image[:, :, :N].reshape(N, N)
    imag = image[:, :, N:].reshape(N, N)
    map_real = maps_ref[0, 0].astype(f32)
    map_imag = maps_ref[0, 1].astype(f32)
    coil_real = (map_real * real - map_imag * imag).astype(bf16)
    coil_imag = (map_real * imag + map_imag * real).astype(bf16)
    coil_image = jnp.concatenate([coil_real, coil_imag], axis=0)
    half = dot(fwd_ref[...], coil_image).astype(bf16)
    half = jnp.concatenate([half[:N], half[N:]], axis=1)
    kspace = dot_nt(fwd_ref[...], half).astype(bf16)
    grid_ref[...] = jnp.zeros_like(grid_ref)

    def visit(group, misfit):
        for copy in copies(group):
            copy.wait()
        wx = wx_ref[group]
        wy = wy_ref[group]
        wy_wide = wy.astype(f32)
        across = dot(kspace, wx)
        weighted = []
        for part in range(2):
            predicted = jnp.sum(across[part * N : (part + 1) * N] * wy_wide, axis=0, keepdims=True)
            resid = []
            for member in range(GROUP):
                block = group * GROUP + member
                measured = samples_ref[0, 0, block].astype(f32)[part : part + 1]
                off = predicted[:, member * BS : (member + 1) * BS] - measured
                resid.append(jnp.where(block < count, off, 0.0))
            resid = jnp.concatenate(resid, axis=1)
            misfit = misfit + resid * resid
            weighted.append(wy * resid.astype(bf16))
        weighted = jnp.concatenate(weighted, axis=0)
        grid_ref[...] += dot_nt(weighted, wx)
        return misfit

    misfit = lax.fori_loop(0, groups, visit, jnp.zeros((1, GS), f32))
    misfit = jnp.broadcast_to(jnp.sum(misfit, axis=1, keepdims=True), (8, 128))

    grid = jnp.concatenate([grid_ref[:N].astype(bf16), -grid_ref[N:].astype(bf16)], axis=1)
    back_half = dot_nt(fwd_ref[...], grid)
    back_half = jnp.concatenate([back_half[:N].astype(bf16), -back_half[N:].astype(bf16)], axis=1)
    back = dot(back_half, fwd_ref[...])
    back_real = back[:, :N]
    back_imag = back[:, N:]
    out_real = map_real * back_real + map_imag * back_imag
    out_imag = map_real * back_imag - map_imag * back_real
    parts = send_ref.shape[0]
    send_ref[:, :, :N] = out_real.reshape(parts, -1, N).astype(bf16)
    send_ref[:, :, N : 2 * N] = out_imag.reshape(parts, -1, N).astype(bf16)
    if last:
        row = lax.broadcasted_iota(jnp.int32, (8, 128), 0)
        extra = jnp.zeros((8, 128), f32)
        for place, piece in enumerate(pieces(before_ref[...]) + pieces(misfit)):
            extra = jnp.where(row == place, piece, extra)
        send_ref[:, :, 2 * N :] = jnp.broadcast_to(extra.astype(bf16)[None], (parts, 8, 128))
    else:
        misfit_ref[...] = misfit


def shrunk(detail, limit):
    real = detail[:, :N]
    imag = detail[:, N:]
    length = jnp.sqrt(real * real + imag * imag)
    factor = jnp.maximum(length - limit, 0.0) / jnp.maximum(length, limit)
    return detail * jnp.concatenate([factor, factor], axis=1)


def unit_change(change):
    real = change[:, :N]
    imag = change[:, N:]
    length = jnp.sqrt(real * real + imag * imag + smooth_floor * smooth_floor)
    return change / jnp.concatenate([length, length], axis=1)


def update_kernel(last, carry_on, misfit_scale, *refs):
    if last:
        (parts_ref, moving_ref, left_ref, right_ref, image_ref, misfit_ref) = refs
    else:
        (parts_ref, moving_ref, left_ref, right_ref, current_ref, send_ref, updated_ref, next_ref) = refs
    total = jnp.sum(parts_ref[...].astype(f32), axis=0)
    moving = moving_ref[...]
    tv_grad = unit_change(moving - left_ref[...]) - unit_change(right_ref[...] - moving)
    field = moving - step_size * (total[:, : 2 * N] + tv_weight * tv_grad)
    rows, width = field.shape
    row_even = lax.broadcasted_iota(jnp.int32, field.shape, 0) % 2 == 0
    col_even = lax.broadcasted_iota(jnp.int32, field.shape, 1) % 2 == 0
    beside = jnp.where(col_even, pltpu.roll(field, width - 1, 1), pltpu.roll(field, 1, 1))
    col_sum = field + beside
    col_diff = jnp.where(col_even, field - beside, beside - field)

    def other_row(values):
        return jnp.where(row_even, pltpu.roll(values, rows - 1, 0), pltpu.roll(values, 1, 0))

    sum_other = other_row(col_sum)
    diff_other = other_row(col_diff)
    limit = step_size * shrink_weight
    approx = (col_sum + sum_other) * 0.5
    horiz = shrunk((col_diff + diff_other) * 0.5, limit)
    vertical = shrunk(jnp.where(row_even, col_sum - sum_other, sum_other - col_sum) * 0.5, limit)
    diagonal = shrunk(jnp.where(row_even, col_diff - diff_other, diff_other - col_diff) * 0.5, limit)
    across = jnp.where(row_even, horiz + diagonal, horiz - diagonal)
    along = jnp.where(row_even, approx + vertical, approx - vertical)
    updated = jnp.where(col_even, along + across, along - across) * 0.5
    if last:
        image_ref[:, 0, 0, :] = updated[:, :N]
        image_ref[:, 0, 1, :] = updated[:, N:]
        extra = total[:, 2 * N :] * misfit_scale
        first = jnp.sum(extra[0:3], axis=0, keepdims=True)
        second = jnp.sum(extra[3:6], axis=0, keepdims=True)
        lane = lax.broadcasted_iota(jnp.int32, first.shape, 1)
        misfit_ref[...] = jnp.where(lane == 0, first, second)[:, :ITERS]
    else:
        following = updated + carry_on * (updated - current_ref[...])
        updated_ref[...] = updated
        next_ref[...] = following
        send_ref[...] = jnp.broadcast_to(following.astype(bf16)[None], send_ref.shape)


def exchanged(parts):
    return lax.all_to_all(parts, "coil", 0, 0, tiled=True)


def neighbours(values):
    count = lax.axis_size("frame")
    left = lax.ppermute(values, "frame", [(i, (i + 1) % count) for i in range(count)])
    right = lax.ppermute(values, "frame", [((i + 1) % count, i) for i in range(count)])
    return left, right


def on_device(
    initial_image,
    coil_maps,
    samples,
    blocks_used,
    row_offset,
    col_offset,
    row_first,
    col_first,
    row_taps,
    col_taps,
):
    coils = lax.axis_size("coil")
    rows = initial_image.shape[0]
    misfit_scale = 0.5 / (coil_maps.shape[0] * coils * NB * BS)
    forward = pair_table(N)
    params = pltpu.CompilerParams(vmem_limit_bytes=32 * 1024 * 1024)
    shape = jax.ShapeDtypeStruct
    send_shape = shape((coils, rows, 2 * N), bf16)
    rows_shape = shape((rows, 2 * N), f32)

    send, moving = pl.pallas_call(
        start_kernel,
        out_shape=(send_shape, rows_shape),
        in_specs=[hbm()],
        out_specs=(vmem(), vmem()),
        scratch_shapes=[pltpu.VMEM(initial_image.shape, f32), pltpu.SemaphoreType.DMA],
        compiler_params=params,
        name="start",
    )(in_hbm(initial_image))
    current = moving

    firsts = (NB, 1, BS)
    weights = pltpu.VMEM((NG, N, GS), bf16)
    wx, wy, forward, maps, measured = pl.pallas_call(
        taps_kernel,
        out_shape=(
            pltpu.HBM((NG, N, GS), bf16),
            pltpu.HBM((NG, N, GS), bf16),
            pltpu.VMEM(forward.shape, bf16),
            pltpu.VMEM(coil_maps.shape, bf16),
            pltpu.VMEM(samples.shape, bf16),
        ),
        in_specs=[smem()] + [hbm() for _ in range(9)],
        out_specs=(hbm(), hbm(), vmem(), vmem(), vmem()),
        scratch_shapes=[
            pltpu.SMEM(row_offset.shape, jnp.int32),
            pltpu.SMEM(col_offset.shape, jnp.int32),
            pltpu.VMEM(firsts, jnp.int32),
            pltpu.VMEM(firsts, jnp.int32),
            pltpu.VMEM(row_taps.shape, bf16),
            pltpu.VMEM(col_taps.shape, bf16),
            weights,
            weights,
            pltpu.SemaphoreType.DMA((9,)),
            pltpu.SemaphoreType.DMA((2, NG)),
        ],
        compiler_params=params,
        name="taps",
    )(
        blocks_used,
        *map(in_hbm, (row_offset, col_offset, row_first.reshape(firsts), col_first.reshape(firsts), row_taps, col_taps)),
        *map(in_hbm, (forward, coil_maps, samples)),
    )

    momentum = 1.0
    misfit = None
    for step_num in range(ITERS):
        last = step_num == ITERS - 1
        gathered = exchanged(send)
        left, right = neighbours(moving)
        if step_num == 0:
            gathered, left, right, wx, wy, forward, maps, measured = lax.optimization_barrier(
                (gathered, left, right, wx, wy, forward, maps, measured)
            )
        else:
            gathered, left, right = lax.optimization_barrier((gathered, left, right))
        inputs = [blocks_used, gathered, maps, measured, forward, in_hbm(wx), in_hbm(wy)]
        specs = [smem(), vmem(), vmem(), vmem(), vmem(), hbm(), hbm()]
        if last:
            inputs.append(misfit)
            specs.append(vmem())
            out_shape = (shape((coils, rows, 2 * N + 128), bf16),)
        else:
            out_shape = (send_shape, shape((8, 128), f32))
        results = pl.pallas_call(
            lambda *refs, last=last: coil_kernel(last, *refs),
            out_shape=out_shape,
            in_specs=specs,
            out_specs=tuple(vmem() for _ in out_shape),
            scratch_shapes=[
                weights,
                weights,
                pltpu.VMEM((2 * N, N), f32),
                pltpu.SemaphoreType.DMA((2, NG)),
            ],
            compiler_params=params,
            name=f"coil{step_num}",
        )(*inputs)
        partial = results[0]
        if not last:
            misfit = results[1]
        parts = exchanged(partial)
        following = (1.0 + math.sqrt(1.0 + 4.0 * momentum * momentum)) / 2.0
        carry_on = (momentum - 1.0) / following
        inputs = [parts, moving, left, right]
        if last:
            out_shape = (shape(initial_image.shape, f32), shape((1, ITERS), f32))
        else:
            inputs.append(current)
            out_shape = (send_shape, rows_shape, rows_shape)
        results = pl.pallas_call(
            lambda *refs, last=last, carry_on=carry_on: update_kernel(last, carry_on, misfit_scale, *refs),
            out_shape=out_shape,
            in_specs=[vmem() for _ in inputs],
            out_specs=tuple(vmem() for _ in out_shape),
            compiler_params=params,
            name=f"update{step_num}",
        )(*inputs)
        if last:
            image, misfit_rows = results
        else:
            send, current, moving = results
        momentum = following
    return image, misfit_rows.T


def solution(mesh):
    placed = (
        P("coil", "frame", None, None),
        P("coil", None, None, None),
        P("coil", "frame", None, None, None),
        P("frame"),
        P("frame", None),
        P("frame", None),
        P("frame", None, None),
        P("frame", None, None),
        P("frame", None, None, None),
        P("frame", None, None, None),
    )
    return jax.shard_map(
        on_device,
        mesh=mesh,
        in_specs=placed,
        out_specs=(P("coil", "frame", None, None), P(None, "frame")),
        check_vma=False,
    )
```

```python
import math

import jax
import jax.numpy as jnp
import numpy as np
from jax import lax
from jax.experimental import pallas as pl
from jax.experimental.pallas import tpu as pltpu
from jax.sharding import PartitionSpec as P

N = 256
NB = 18
BS = 256
KW = 4
ITERS = 2
TT = 128
GROUP = 6
NG = NB // GROUP
ALIGN = 16
WINDOW = TT + ALIGN

step_size = 2.0
tv_weight = 0.1
smooth_floor = 0.5
shrink_weight = 0.1

f32 = jnp.float32
bf16 = jnp.bfloat16


def pair_table(order):
    counter = np.arange(order)
    phase = (counter[:, None] * counter[None, :]) % order
    angle = phase.astype(np.float32) * np.float32(2.0 * math.pi / order)
    cosine = np.cos(angle) / np.float32(math.sqrt(order))
    sine = np.sin(angle) / np.float32(math.sqrt(order))
    return jnp.asarray(np.block([[cosine, sine], [-sine, cosine]]), bf16)


def vmem():
    return pl.BlockSpec(memory_space=pltpu.VMEM)


def smem():
    return pl.BlockSpec(memory_space=pltpu.SMEM)


def hbm():
    return pl.BlockSpec(memory_space=pltpu.HBM)


def in_hbm(values):
    return pltpu.with_memory_space_constraint(values, pltpu.HBM)


def dot(left, right):
    return lax.dot_general(left, right, (((1,), (0,)), ((), ())), preferred_element_type=f32)


def dot_nt(left, right):
    return lax.dot_general(left, right, (((1,), (1,)), ((), ())), preferred_element_type=f32)


def start_kernel(image_hbm, send_ref, rows_ref, image_ref, sem):
    copy = pltpu.make_async_copy(image_hbm, image_ref, sem)
    copy.start()
    copy.wait()
    real = image_ref[:, 0, 0, :]
    imag = image_ref[:, 0, 1, :]
    rows_ref[:, :N] = real
    rows_ref[:, N:] = imag
    low = jnp.concatenate([real, imag], axis=1).astype(bf16)
    send_ref[...] = jnp.broadcast_to(low[None], send_ref.shape)


def window_start(offset):
    return pl.multiple_of(jnp.minimum((offset >> 4) << 4, N - WINDOW), ALIGN)


def taps_kernel(count_ref, row_off, col_off, *refs):
    sources, (wx_hbm, wy_hbm, wx_keep, wy_keep), kept, held = refs[:7], refs[7:11], refs[11:14], refs[14:18]
    wx_ref, wy_ref, in_sems, out_sems = refs[18:]
    row_first, col_first, row_taps, col_taps = held
    loads = [pltpu.make_async_copy(source, own, in_sems.at[k]) for k, (source, own) in enumerate(zip(sources, held + kept))]
    for load in loads:
        load.start()
    for load in loads[: len(held)]:
        load.wait()
    groups = (count_ref[0] + GROUP - 1) // GROUP

    def stores(group):
        blocks = pl.ds(group * GROUP - GROUP, GROUP)
        return (
            pltpu.make_async_copy(wx_ref.at[blocks], wx_hbm.at[blocks], out_sems.at[0, group]),
            pltpu.make_async_copy(wy_ref.at[blocks], wy_hbm.at[blocks], out_sems.at[1, group]),
        )

    def matrix(length, start, taps):
        offset = lax.broadcasted_iota(jnp.int32, (length, BS), 0) - start
        values = jnp.zeros((length, BS), f32)
        for tap in range(KW):
            values = jnp.where(offset == tap, taps[tap : tap + 1], values)
        return values.astype(bf16)

    def build(block, wx_out, wy_out, place):
        col = col_off[block]
        wx_out[place] = matrix(N, row_first[block] + row_off[block], row_taps[0, block].astype(f32))
        wy_out[place] = matrix(WINDOW, col_first[block] + (col - window_start(col)), col_taps[0, block].astype(f32))

    def first(block, carry):
        build(block, wx_keep, wy_keep, block)
        return carry

    def visit(group, carry):
        for member in range(GROUP):
            block = group * GROUP + member
            build(block, wx_ref, wy_ref, block - GROUP)
        for store in stores(group):
            store.start()
        return carry

    def finish(group, carry):
        for store in stores(group):
            store.wait()
        return carry

    lax.fori_loop(1, groups, visit, 0)
    lax.fori_loop(0, GROUP, first, 0)
    lax.fori_loop(1, groups, finish, 0)
    for load in loads[len(held) :]:
        load.wait()


def pieces(value):
    high = value.astype(bf16)
    rest = value - high.astype(f32)
    middle = rest.astype(bf16)
    low = (rest - middle.astype(f32)).astype(bf16)
    return high.astype(f32), middle.astype(f32), low.astype(f32)


def coil_kernel(last, *refs):
    (count_ref, col_off, image_ref, maps_ref, samples_ref, fwd_ref, wx_keep, wy_keep, wx_hbm, wy_hbm) = refs[:10]
    if last:
        (before_ref, send_ref) = refs[10:12]
    else:
        (send_ref, misfit_ref) = refs[10:12]
    (wx_ref, wy_ref, kspace_ref, grid_ref, sems) = refs[12:]
    count = count_ref[0]
    groups = (count + GROUP - 1) // GROUP

    def copies(group):
        blocks = pl.ds(group * GROUP - GROUP, GROUP)
        return (
            pltpu.make_async_copy(wx_hbm.at[blocks], wx_ref.at[blocks], sems.at[0, group]),
            pltpu.make_async_copy(wy_hbm.at[blocks], wy_ref.at[blocks], sems.at[1, group]),
        )

    def fetch(group, carry):
        for copy in copies(group):
            copy.start()
        return carry

    lax.fori_loop(1, groups, fetch, 0)

    image = image_ref[...].astype(f32)
    real = image[:, :, :N].reshape(N, N)
    imag = image[:, :, N:].reshape(N, N)
    map_real = maps_ref[0, 0].astype(f32)
    map_imag = maps_ref[0, 1].astype(f32)
    coil_real = (map_real * real - map_imag * imag).astype(bf16)
    coil_imag = (map_real * imag + map_imag * real).astype(bf16)
    coil_image = jnp.concatenate([coil_real, coil_imag], axis=0)
    half = [dot(fwd_ref[part * N : (part + 1) * N], coil_image).astype(bf16) for part in range(2)]
    half = jnp.concatenate(half, axis=1)
    for part in range(2):
        kspace_ref[part] = dot_nt(fwd_ref[part * N : (part + 1) * N], half).astype(bf16)
    grid_ref[...] = jnp.zeros_like(grid_ref)

    def visit(group, wx_in, wy_in, misfit):
        for member in range(GROUP):
            block = group * GROUP + member
            place = member if wx_in is wx_keep else block - GROUP
            window = pl.ds(window_start(col_off[block]), WINDOW)
            wx = wx_in[place]
            wy = wy_in[place]
            wy_wide = wy.astype(f32)
            measured = samples_ref[0, 0, block].astype(f32)
            tile = jnp.concatenate([kspace_ref[0, window, :], kspace_ref[1, window, :]], axis=0)
            across = dot(tile, wx)
            weighted = []
            for part in range(2):
                predicted = jnp.sum(across[part * WINDOW : (part + 1) * WINDOW] * wy_wide, axis=0, keepdims=True)
                resid = jnp.where(block < count, predicted - measured[part : part + 1], 0.0)
                misfit = misfit + resid * resid
                weighted.append(wy * resid.astype(bf16))
            spread = dot_nt(jnp.concatenate(weighted, axis=0), wx)
            for part in range(2):
                grid_ref[part, window, :] += spread[part * WINDOW : (part + 1) * WINDOW]
        return misfit

    def later(group, misfit):
        for copy in copies(group):
            copy.wait()
        return visit(group, wx_ref, wy_ref, misfit)

    misfit = visit(0, wx_keep, wy_keep, jnp.zeros((1, BS), f32))
    misfit = lax.fori_loop(1, groups, later, misfit)
    misfit = jnp.broadcast_to(jnp.sum(misfit, axis=1, keepdims=True), (8, 128))

    grid_real = grid_ref[0].astype(bf16)
    grid_imag = grid_ref[1].astype(bf16)
    grid = jnp.concatenate([grid_real, -grid_imag], axis=1)
    back_real = dot_nt(fwd_ref[:N], grid).astype(bf16)
    back_imag = dot_nt(fwd_ref[N:], grid).astype(bf16)
    back_half = jnp.concatenate([back_real, -back_imag], axis=1)
    back = dot(back_half, fwd_ref[...])
    back_real = back[:, :N]
    back_imag = back[:, N:]
    map_real = maps_ref[0, 0].astype(f32)
    map_imag = maps_ref[0, 1].astype(f32)
    out_real = map_real * back_real + map_imag * back_imag
    out_imag = map_real * back_imag - map_imag * back_real
    parts = send_ref.shape[0]
    send_ref[:, :, :N] = out_real.reshape(parts, -1, N).astype(bf16)
    send_ref[:, :, N : 2 * N] = out_imag.reshape(parts, -1, N).astype(bf16)
    if last:
        row = lax.broadcasted_iota(jnp.int32, (8, 128), 0)
        extra = jnp.zeros((8, 128), f32)
        for place, piece in enumerate(pieces(before_ref[...]) + pieces(misfit)):
            extra = jnp.where(row == place, piece, extra)
        send_ref[:, :, 2 * N :] = jnp.broadcast_to(extra.astype(bf16)[None], (parts, 8, 128))
    else:
        misfit_ref[...] = misfit


def shrunk(detail, limit):
    real = detail[:, :N]
    imag = detail[:, N:]
    length = jnp.sqrt(real * real + imag * imag)
    factor = jnp.maximum(length - limit, 0.0) / jnp.maximum(length, limit)
    return detail * jnp.concatenate([factor, factor], axis=1)


def unit_change(change):
    real = change[:, :N]
    imag = change[:, N:]
    length = jnp.sqrt(real * real + imag * imag + smooth_floor * smooth_floor)
    return change / jnp.concatenate([length, length], axis=1)


def update_kernel(last, carry_on, misfit_scale, *refs):
    if last:
        (parts_ref, moving_ref, left_ref, right_ref, image_ref, misfit_ref) = refs
    else:
        (parts_ref, moving_ref, left_ref, right_ref, current_ref, send_ref, next_ref) = refs
    total = jnp.sum(parts_ref[...].astype(f32), axis=0)
    moving = moving_ref[...]
    tv_grad = unit_change(moving - left_ref[...]) - unit_change(right_ref[...] - moving)
    field = moving - step_size * (total[:, : 2 * N] + tv_weight * tv_grad)
    rows, width = field.shape
    row_even = lax.broadcasted_iota(jnp.int32, field.shape, 0) % 2 == 0
    col_even = lax.broadcasted_iota(jnp.int32, field.shape, 1) % 2 == 0
    beside = jnp.where(col_even, pltpu.roll(field, width - 1, 1), pltpu.roll(field, 1, 1))
    col_sum = field + beside
    col_diff = jnp.where(col_even, field - beside, beside - field)

    def other_row(values):
        return jnp.where(row_even, pltpu.roll(values, rows - 1, 0), pltpu.roll(values, 1, 0))

    sum_other = other_row(col_sum)
    diff_other = other_row(col_diff)
    limit = step_size * shrink_weight
    approx = (col_sum + sum_other) * 0.5
    horiz = shrunk((col_diff + diff_other) * 0.5, limit)
    vertical = shrunk(jnp.where(row_even, col_sum - sum_other, sum_other - col_sum) * 0.5, limit)
    diagonal = shrunk(jnp.where(row_even, col_diff - diff_other, diff_other - col_diff) * 0.5, limit)
    across = jnp.where(row_even, horiz + diagonal, horiz - diagonal)
    along = jnp.where(row_even, approx + vertical, approx - vertical)
    updated = jnp.where(col_even, along + across, along - across) * 0.5
    if last:
        image_ref[:, 0, 0, :] = updated[:, :N]
        image_ref[:, 0, 1, :] = updated[:, N:]
        extra = total[:, 2 * N :] * misfit_scale
        first = jnp.sum(extra[0:3], axis=0, keepdims=True)
        second = jnp.sum(extra[3:6], axis=0, keepdims=True)
        lane = lax.broadcasted_iota(jnp.int32, first.shape, 1)
        misfit_ref[...] = jnp.where(lane == 0, first, second)[:, :ITERS]
    else:
        following = updated + carry_on * (updated - current_ref[...])
        next_ref[...] = following
        send_ref[...] = jnp.broadcast_to(following.astype(bf16)[None], send_ref.shape)


def exchanged(parts):
    return lax.all_to_all(parts, "coil", 0, 0, tiled=True)


def neighbours(values):
    count = lax.axis_size("frame")
    left = lax.ppermute(values, "frame", [(i, (i + 1) % count) for i in range(count)])
    right = lax.ppermute(values, "frame", [((i + 1) % count, i) for i in range(count)])
    return left, right


def on_device(
    initial_image,
    coil_maps,
    samples,
    blocks_used,
    row_offset,
    col_offset,
    row_first,
    col_first,
    row_taps,
    col_taps,
):
    coils = lax.axis_size("coil")
    rows = initial_image.shape[0]
    misfit_scale = 0.5 / (coil_maps.shape[0] * coils * NB * BS)
    forward = pair_table(N)
    params = pltpu.CompilerParams(vmem_limit_bytes=32 * 1024 * 1024)
    shape = jax.ShapeDtypeStruct
    send_shape = pltpu.VMEM((coils, rows, 2 * N), bf16)
    rows_shape = pltpu.VMEM((rows, 2 * N), f32)

    send, moving = pl.pallas_call(
        start_kernel,
        out_shape=(send_shape, rows_shape),
        in_specs=[hbm()],
        out_specs=(vmem(), vmem()),
        scratch_shapes=[pltpu.VMEM(initial_image.shape, f32), pltpu.SemaphoreType.DMA],
        compiler_params=params,
        name="start",
    )(in_hbm(initial_image))
    initial = moving

    firsts = (NB, 1, BS)
    wx_shape = (NB - GROUP, N, BS)
    wy_shape = (NB - GROUP, WINDOW, BS)
    row_off = row_offset.reshape(NB)
    col_off = col_offset.reshape(NB)
    constants = pl.pallas_call(
        taps_kernel,
        out_shape=(
            pltpu.HBM(wx_shape, bf16),
            pltpu.HBM(wy_shape, bf16),
            pltpu.VMEM((GROUP, N, BS), bf16),
            pltpu.VMEM((GROUP, WINDOW, BS), bf16),
            pltpu.VMEM(forward.shape, bf16),
            pltpu.VMEM(coil_maps.shape, bf16),
            pltpu.VMEM(samples.shape, bf16),
        ),
        in_specs=[smem(), smem(), smem()] + [hbm() for _ in range(7)],
        out_specs=(hbm(), hbm(), vmem(), vmem(), vmem(), vmem(), vmem()),
        scratch_shapes=[
            pltpu.VMEM(firsts, jnp.int32),
            pltpu.VMEM(firsts, jnp.int32),
            pltpu.VMEM(row_taps.shape, bf16),
            pltpu.VMEM(col_taps.shape, bf16),
            pltpu.VMEM(wx_shape, bf16),
            pltpu.VMEM(wy_shape, bf16),
            pltpu.SemaphoreType.DMA((7,)),
            pltpu.SemaphoreType.DMA((2, NG)),
        ],
        compiler_params=params,
        name="taps",
    )(
        blocks_used,
        row_off,
        col_off,
        *map(in_hbm, (row_first.reshape(firsts), col_first.reshape(firsts), row_taps, col_taps)),
        *map(in_hbm, (forward, coil_maps, samples)),
    )

    momentum = 1.0
    misfit = None
    for step_num in range(ITERS):
        last = step_num == ITERS - 1
        gathered = exchanged(send)
        left, right = neighbours(moving)
        if step_num == 0:
            gathered, left, right, constants = lax.optimization_barrier((gathered, left, right, constants))
            wx, wy, wx_keep, wy_keep, forward, maps, measured = constants
        else:
            gathered, left, right = lax.optimization_barrier((gathered, left, right))
        inputs = [blocks_used, col_off, gathered, maps, measured, forward, wx_keep, wy_keep, in_hbm(wx), in_hbm(wy)]
        specs = [smem(), smem()] + [vmem() for _ in range(6)] + [hbm(), hbm()]
        if last:
            inputs.append(misfit)
            specs.append(vmem())
            out_shape = (pltpu.VMEM((coils, rows, 2 * N + 128), bf16),)
        else:
            out_shape = (send_shape, shape((8, 128), f32))
        results = pl.pallas_call(
            lambda *refs, last=last: coil_kernel(last, *refs),
            out_shape=out_shape,
            in_specs=specs,
            out_specs=tuple(vmem() for _ in out_shape),
            scratch_shapes=[
                pltpu.VMEM(wx_shape, bf16),
                pltpu.VMEM(wy_shape, bf16),
                pltpu.VMEM((2, N, N), bf16),
                pltpu.VMEM((2, N, N), f32),
                pltpu.SemaphoreType.DMA((2, NG)),
            ],
            compiler_params=params,
            name=f"coil{step_num}",
        )(*inputs)
        partial = results[0]
        if not last:
            misfit = results[1]
        parts = exchanged(partial)
        following = (1.0 + math.sqrt(1.0 + 4.0 * momentum * momentum)) / 2.0
        carry_on = (momentum - 1.0) / following
        inputs = [parts, moving, left, right]
        if last:
            out_shape = (shape(initial_image.shape, f32), shape((1, ITERS), f32))
        else:
            inputs.append(initial)
            out_shape = (send_shape, rows_shape)
        results = pl.pallas_call(
            lambda *refs, last=last, carry_on=carry_on: update_kernel(last, carry_on, misfit_scale, *refs),
            out_shape=out_shape,
            in_specs=[vmem() for _ in inputs],
            out_specs=tuple(vmem() for _ in out_shape),
            compiler_params=params,
            name=f"update{step_num}",
        )(*inputs)
        if last:
            image, misfit_rows = results
        else:
            send, moving = results
        momentum = following
    return image, misfit_rows.T


def solution(mesh):
    placed = (
        P("coil", "frame", None, None),
        P("coil", None, None, None),
        P("coil", "frame", None, None, None),
        P("frame"),
        P("frame", None),
        P("frame", None),
        P("frame", None, None),
        P("frame", None, None),
        P("frame", None, None, None),
        P("frame", None, None, None),
    )
    return jax.shard_map(
        on_device,
        mesh=mesh,
        in_specs=placed,
        out_specs=(P("coil", "frame", None, None), P(None, "frame")),
        check_vma=False,
    )
```

```python
import math

import jax
import jax.numpy as jnp
import numpy as np
from jax import lax
from jax.experimental import pallas as pl
from jax.experimental.pallas import tpu as pltpu
from jax.sharding import PartitionSpec as P

N = 256
NB = 18
BS = 256
KW = 4
ITERS = 2
TT = 128
GROUP = 6
NG = NB // GROUP
ALIGN = 16
WINDOW = TT + ALIGN

step_size = 2.0
tv_weight = 0.1
smooth_floor = 0.5
shrink_weight = 0.1

f32 = jnp.float32
bf16 = jnp.bfloat16


def pair_table(order):
    counter = np.arange(order)
    phase = (counter[:, None] * counter[None, :]) % order
    angle = phase.astype(np.float32) * np.float32(2.0 * math.pi / order)
    cosine = np.cos(angle) / np.float32(math.sqrt(order))
    sine = np.sin(angle) / np.float32(math.sqrt(order))
    return jnp.asarray(np.block([[cosine, sine], [-sine, cosine]]), bf16)


def vmem():
    return pl.BlockSpec(memory_space=pltpu.VMEM)


def smem():
    return pl.BlockSpec(memory_space=pltpu.SMEM)


def hbm():
    return pl.BlockSpec(memory_space=pltpu.HBM)


def in_hbm(values):
    return pltpu.with_memory_space_constraint(values, pltpu.HBM)


def dot(left, right):
    return lax.dot_general(left, right, (((1,), (0,)), ((), ())), preferred_element_type=f32)


def dot_nt(left, right):
    return lax.dot_general(left, right, (((1,), (1,)), ((), ())), preferred_element_type=f32)


def start_kernel(image_hbm, send_ref, rows_ref, image_ref, sem):
    copy = pltpu.make_async_copy(image_hbm, image_ref, sem)
    copy.start()
    copy.wait()
    real = image_ref[:, 0, 0, :]
    imag = image_ref[:, 0, 1, :]
    rows_ref[:, :N] = real
    rows_ref[:, N:] = imag
    low = jnp.concatenate([real, imag], axis=1).astype(bf16)
    send_ref[...] = jnp.broadcast_to(low[None], send_ref.shape)


def window_start(offset):
    return pl.multiple_of(jnp.minimum((offset >> 4) << 4, N - WINDOW), ALIGN)


def taps_kernel(count_ref, *refs):
    sources, (wx_hbm, wy_hbm, wx_keep, wy_keep), kept, held = refs[:9], refs[9:13], refs[13:16], refs[16:22]
    wx_ref, wy_ref, in_sems, out_sems = refs[22:]
    row_off, col_off, row_first, col_first, row_taps, col_taps = held
    loads = [pltpu.make_async_copy(source, own, in_sems.at[k]) for k, (source, own) in enumerate(zip(sources, held + kept))]
    for load in loads:
        load.start()
    for load in loads[: len(held)]:
        load.wait()
    groups = (count_ref[0] + GROUP - 1) // GROUP

    def stores(group):
        blocks = pl.ds(group * GROUP - GROUP, GROUP)
        return (
            pltpu.make_async_copy(wx_ref.at[blocks], wx_hbm.at[blocks], out_sems.at[0, group]),
            pltpu.make_async_copy(wy_ref.at[blocks], wy_hbm.at[blocks], out_sems.at[1, group]),
        )

    def matrix(length, start, taps):
        offset = lax.broadcasted_iota(jnp.int32, (length, BS), 0) - start
        values = jnp.zeros((length, BS), f32)
        for tap in range(KW):
            values = jnp.where(offset == tap, taps[tap : tap + 1], values)
        return values.astype(bf16)

    def build(block, wx_out, wy_out, place):
        col = col_off[0, block]
        wx_out[place] = matrix(N, row_first[block] + row_off[0, block], row_taps[0, block].astype(f32))
        wy_out[place] = matrix(WINDOW, col_first[block] + (col - window_start(col)), col_taps[0, block].astype(f32))

    def first(block, carry):
        build(block, wx_keep, wy_keep, block)
        return carry

    def visit(group, carry):
        for member in range(GROUP):
            block = group * GROUP + member
            build(block, wx_ref, wy_ref, block - GROUP)
        for store in stores(group):
            store.start()
        return carry

    def finish(group, carry):
        for store in stores(group):
            store.wait()
        return carry

    lax.fori_loop(1, groups, visit, 0)
    lax.fori_loop(0, GROUP, first, 0)
    lax.fori_loop(1, groups, finish, 0)
    for load in loads[len(held) :]:
        load.wait()


def pieces(value):
    high = value.astype(bf16)
    rest = value - high.astype(f32)
    middle = rest.astype(bf16)
    low = (rest - middle.astype(f32)).astype(bf16)
    return high.astype(f32), middle.astype(f32), low.astype(f32)


def coil_kernel(last, *refs):
    (count_ref, image_ref, maps_ref, samples_ref, fwd_ref, wx_keep, wy_keep, wx_hbm, wy_hbm, col_off_hbm) = refs[:10]
    if last:
        (before_ref, send_ref) = refs[10:12]
    else:
        (send_ref, misfit_ref) = refs[10:12]
    (col_off, wx_ref, wy_ref, kspace_ref, grid_ref, sems, off_sem) = refs[12:]
    count = count_ref[0]
    groups = (count + GROUP - 1) // GROUP

    def copies(group):
        blocks = pl.ds(group * GROUP - GROUP, GROUP)
        return (
            pltpu.make_async_copy(wx_hbm.at[blocks], wx_ref.at[blocks], sems.at[0, group]),
            pltpu.make_async_copy(wy_hbm.at[blocks], wy_ref.at[blocks], sems.at[1, group]),
        )

    def fetch(group, carry):
        for copy in copies(group):
            copy.start()
        return carry

    off_copy = pltpu.make_async_copy(col_off_hbm, col_off, off_sem)
    off_copy.start()
    lax.fori_loop(1, groups, fetch, 0)

    image = image_ref[...].astype(f32)
    real = image[:, :, :N].reshape(N, N)
    imag = image[:, :, N:].reshape(N, N)
    map_real = maps_ref[0, 0].astype(f32)
    map_imag = maps_ref[0, 1].astype(f32)
    coil_real = (map_real * real - map_imag * imag).astype(bf16)
    coil_imag = (map_real * imag + map_imag * real).astype(bf16)
    coil_image = jnp.concatenate([coil_real, coil_imag], axis=0)
    half = [dot(fwd_ref[part * N : (part + 1) * N], coil_image).astype(bf16) for part in range(2)]
    half = jnp.concatenate(half, axis=1)
    for part in range(2):
        kspace_ref[part] = dot_nt(fwd_ref[part * N : (part + 1) * N], half).astype(bf16)
    grid_ref[...] = jnp.zeros_like(grid_ref)

    def visit(group, wx_in, wy_in, misfit):
        for member in range(GROUP):
            block = group * GROUP + member
            place = member if wx_in is wx_keep else block - GROUP
            window = pl.ds(window_start(col_off[0, block]), WINDOW)
            wx = wx_in[place]
            wy = wy_in[place]
            wy_wide = wy.astype(f32)
            measured = samples_ref[0, 0, block].astype(f32)
            tile = jnp.concatenate([kspace_ref[0, window, :], kspace_ref[1, window, :]], axis=0)
            across = dot(tile, wx)
            weighted = []
            for part in range(2):
                predicted = jnp.sum(across[part * WINDOW : (part + 1) * WINDOW] * wy_wide, axis=0, keepdims=True)
                resid = jnp.where(block < count, predicted - measured[part : part + 1], 0.0)
                misfit = misfit + resid * resid
                weighted.append(wy * resid.astype(bf16))
            spread = dot_nt(jnp.concatenate(weighted, axis=0), wx)
            for part in range(2):
                grid_ref[part, window, :] += spread[part * WINDOW : (part + 1) * WINDOW]
        return misfit

    def later(group, misfit):
        for copy in copies(group):
            copy.wait()
        return visit(group, wx_ref, wy_ref, misfit)

    off_copy.wait()
    misfit = visit(0, wx_keep, wy_keep, jnp.zeros((1, BS), f32))
    misfit = lax.fori_loop(1, groups, later, misfit)
    misfit = jnp.broadcast_to(jnp.sum(misfit, axis=1, keepdims=True), (8, 128))

    grid_real = grid_ref[0].astype(bf16)
    grid_imag = grid_ref[1].astype(bf16)
    grid = jnp.concatenate([grid_real, -grid_imag], axis=1)
    back_real = dot_nt(fwd_ref[:N], grid).astype(bf16)
    back_imag = dot_nt(fwd_ref[N:], grid).astype(bf16)
    back_half = jnp.concatenate([back_real, -back_imag], axis=1)
    back = dot(back_half, fwd_ref[...])
    back_real = back[:, :N]
    back_imag = back[:, N:]
    map_real = maps_ref[0, 0].astype(f32)
    map_imag = maps_ref[0, 1].astype(f32)
    out_real = map_real * back_real + map_imag * back_imag
    out_imag = map_real * back_imag - map_imag * back_real
    parts = send_ref.shape[0]
    send_ref[:, :, :N] = out_real.reshape(parts, -1, N).astype(bf16)
    send_ref[:, :, N : 2 * N] = out_imag.reshape(parts, -1, N).astype(bf16)
    if last:
        row = lax.broadcasted_iota(jnp.int32, (8, 128), 0)
        extra = jnp.zeros((8, 128), f32)
        for place, piece in enumerate(pieces(before_ref[...]) + pieces(misfit)):
            extra = jnp.where(row == place, piece, extra)
        send_ref[:, :, 2 * N :] = jnp.broadcast_to(extra.astype(bf16)[None], (parts, 8, 128))
    else:
        misfit_ref[...] = misfit


def shrunk(detail, limit):
    real = detail[:, :N]
    imag = detail[:, N:]
    length = jnp.sqrt(real * real + imag * imag)
    factor = jnp.maximum(length - limit, 0.0) / jnp.maximum(length, limit)
    return detail * jnp.concatenate([factor, factor], axis=1)


def unit_change(change):
    real = change[:, :N]
    imag = change[:, N:]
    length = jnp.sqrt(real * real + imag * imag + smooth_floor * smooth_floor)
    return change / jnp.concatenate([length, length], axis=1)


def update_kernel(last, carry_on, misfit_scale, *refs):
    if last:
        (parts_ref, moving_ref, left_ref, right_ref, image_ref, misfit_ref) = refs
    else:
        (parts_ref, moving_ref, left_ref, right_ref, current_ref, send_ref, next_ref) = refs
    total = jnp.sum(parts_ref[...].astype(f32), axis=0)
    moving = moving_ref[...]
    tv_grad = unit_change(moving - left_ref[...]) - unit_change(right_ref[...] - moving)
    field = moving - step_size * (total[:, : 2 * N] + tv_weight * tv_grad)
    rows, width = field.shape
    row_even = lax.broadcasted_iota(jnp.int32, field.shape, 0) % 2 == 0
    col_even = lax.broadcasted_iota(jnp.int32, field.shape, 1) % 2 == 0
    beside = jnp.where(col_even, pltpu.roll(field, width - 1, 1), pltpu.roll(field, 1, 1))
    col_sum = field + beside
    col_diff = jnp.where(col_even, field - beside, beside - field)

    def other_row(values):
        return jnp.where(row_even, pltpu.roll(values, rows - 1, 0), pltpu.roll(values, 1, 0))

    sum_other = other_row(col_sum)
    diff_other = other_row(col_diff)
    limit = step_size * shrink_weight
    approx = (col_sum + sum_other) * 0.5
    horiz = shrunk((col_diff + diff_other) * 0.5, limit)
    vertical = shrunk(jnp.where(row_even, col_sum - sum_other, sum_other - col_sum) * 0.5, limit)
    diagonal = shrunk(jnp.where(row_even, col_diff - diff_other, diff_other - col_diff) * 0.5, limit)
    across = jnp.where(row_even, horiz + diagonal, horiz - diagonal)
    along = jnp.where(row_even, approx + vertical, approx - vertical)
    updated = jnp.where(col_even, along + across, along - across) * 0.5
    if last:
        image_ref[:, 0, 0, :] = updated[:, :N]
        image_ref[:, 0, 1, :] = updated[:, N:]
        extra = total[:, 2 * N :] * misfit_scale
        first = jnp.sum(extra[0:3], axis=0, keepdims=True)
        second = jnp.sum(extra[3:6], axis=0, keepdims=True)
        lane = lax.broadcasted_iota(jnp.int32, first.shape, 1)
        misfit_ref[...] = jnp.where(lane == 0, first, second)[:, :ITERS]
    else:
        following = updated + carry_on * (updated - current_ref[...])
        next_ref[...] = following
        send_ref[...] = jnp.broadcast_to(following.astype(bf16)[None], send_ref.shape)


def exchanged(parts):
    return lax.all_to_all(parts, "coil", 0, 0, tiled=True)


def neighbours(values):
    count = lax.axis_size("frame")
    left = lax.ppermute(values, "frame", [(i, (i + 1) % count) for i in range(count)])
    right = lax.ppermute(values, "frame", [((i + 1) % count, i) for i in range(count)])
    return left, right


def on_device(
    initial_image,
    coil_maps,
    samples,
    blocks_used,
    row_offset,
    col_offset,
    row_first,
    col_first,
    row_taps,
    col_taps,
):
    coils = lax.axis_size("coil")
    rows = initial_image.shape[0]
    misfit_scale = 0.5 / (coil_maps.shape[0] * coils * NB * BS)
    forward = pair_table(N)
    params = pltpu.CompilerParams(vmem_limit_bytes=32 * 1024 * 1024)
    shape = jax.ShapeDtypeStruct
    send_shape = pltpu.VMEM((coils, rows, 2 * N), bf16)
    rows_shape = pltpu.VMEM((rows, 2 * N), f32)

    send, moving = pl.pallas_call(
        start_kernel,
        out_shape=(send_shape, rows_shape),
        in_specs=[hbm()],
        out_specs=(vmem(), vmem()),
        scratch_shapes=[pltpu.VMEM(initial_image.shape, f32), pltpu.SemaphoreType.DMA],
        compiler_params=params,
        name="start",
    )(in_hbm(initial_image))
    initial = moving

    firsts = (NB, 1, BS)
    wx_shape = (NB - GROUP, N, BS)
    wy_shape = (NB - GROUP, WINDOW, BS)
    constants = pl.pallas_call(
        taps_kernel,
        out_shape=(
            pltpu.HBM(wx_shape, bf16),
            pltpu.HBM(wy_shape, bf16),
            pltpu.VMEM((GROUP, N, BS), bf16),
            pltpu.VMEM((GROUP, WINDOW, BS), bf16),
            pltpu.VMEM(forward.shape, bf16),
            pltpu.VMEM(coil_maps.shape, bf16),
            pltpu.VMEM(samples.shape, bf16),
        ),
        in_specs=[smem()] + [hbm() for _ in range(9)],
        out_specs=(hbm(), hbm(), vmem(), vmem(), vmem(), vmem(), vmem()),
        scratch_shapes=[
            pltpu.SMEM(row_offset.shape, jnp.int32),
            pltpu.SMEM(col_offset.shape, jnp.int32),
            pltpu.VMEM(firsts, jnp.int32),
            pltpu.VMEM(firsts, jnp.int32),
            pltpu.VMEM(row_taps.shape, bf16),
            pltpu.VMEM(col_taps.shape, bf16),
            pltpu.VMEM(wx_shape, bf16),
            pltpu.VMEM(wy_shape, bf16),
            pltpu.SemaphoreType.DMA((9,)),
            pltpu.SemaphoreType.DMA((2, NG)),
        ],
        compiler_params=params,
        name="taps",
    )(
        blocks_used,
        *map(in_hbm, (row_offset, col_offset, row_first.reshape(firsts), col_first.reshape(firsts), row_taps, col_taps)),
        *map(in_hbm, (forward, coil_maps, samples)),
    )

    momentum = 1.0
    misfit = None
    for step_num in range(ITERS):
        last = step_num == ITERS - 1
        gathered = exchanged(send)
        left, right = neighbours(moving)
        if step_num == 0:
            gathered, left, right, constants = lax.optimization_barrier((gathered, left, right, constants))
            wx, wy, wx_keep, wy_keep, forward, maps, measured = constants
        else:
            gathered, left, right = lax.optimization_barrier((gathered, left, right))
        inputs = [blocks_used, gathered, maps, measured, forward, wx_keep, wy_keep, *map(in_hbm, (wx, wy, col_offset))]
        specs = [smem()] + [vmem() for _ in range(6)] + [hbm() for _ in range(3)]
        if last:
            inputs.append(misfit)
            specs.append(vmem())
            out_shape = (pltpu.VMEM((coils, rows, 2 * N + 128), bf16),)
        else:
            out_shape = (send_shape, shape((8, 128), f32))
        results = pl.pallas_call(
            lambda *refs, last=last: coil_kernel(last, *refs),
            out_shape=out_shape,
            in_specs=specs,
            out_specs=tuple(vmem() for _ in out_shape),
            scratch_shapes=[
                pltpu.SMEM(col_offset.shape, jnp.int32),
                pltpu.VMEM(wx_shape, bf16),
                pltpu.VMEM(wy_shape, bf16),
                pltpu.VMEM((2, N, N), bf16),
                pltpu.VMEM((2, N, N), f32),
                pltpu.SemaphoreType.DMA((2, NG)),
                pltpu.SemaphoreType.DMA,
            ],
            compiler_params=params,
            name=f"coil{step_num}",
        )(*inputs)
        partial = results[0]
        if not last:
            misfit = results[1]
        parts = exchanged(partial)
        following = (1.0 + math.sqrt(1.0 + 4.0 * momentum * momentum)) / 2.0
        carry_on = (momentum - 1.0) / following
        inputs = [parts, moving, left, right]
        if last:
            out_shape = (shape(initial_image.shape, f32), shape((1, ITERS), f32))
        else:
            inputs.append(initial)
            out_shape = (send_shape, rows_shape)
        results = pl.pallas_call(
            lambda *refs, last=last, carry_on=carry_on: update_kernel(last, carry_on, misfit_scale, *refs),
            out_shape=out_shape,
            in_specs=[vmem() for _ in inputs],
            out_specs=tuple(vmem() for _ in out_shape),
            compiler_params=params,
            name=f"update{step_num}",
        )(*inputs)
        if last:
            image, misfit_rows = results
        else:
            send, moving = results
        momentum = following
    return image, misfit_rows.T


def solution(mesh):
    placed = (
        P("coil", "frame", None, None),
        P("coil", None, None, None),
        P("coil", "frame", None, None, None),
        P("frame"),
        P("frame", None),
        P("frame", None),
        P("frame", None, None),
        P("frame", None, None),
        P("frame", None, None, None),
        P("frame", None, None, None),
    )
    return jax.shard_map(
        on_device,
        mesh=mesh,
        in_specs=placed,
        out_specs=(P("coil", "frame", None, None), P(None, "frame")),
        check_vma=False,
    )
```
